32 devices in a mesh: slab: 8 (over z, y), plane: 4 (over x, core).
Axes of the slice: x: 2, y: 2, z: 4, core: 2. Of those that a mesh axis runs over, the one named last changes fastest.
Arguments:
- tissue_v: float32 [32, 64, 128], P('slab', 'plane'), may hold values from -4 to 4
- tissue_gates: float32 [40, 32, 64, 128], P(None, 'slab', 'plane'), may hold values from 0 to 1
- tissue_diff: float32 [32, 64, 128], P('slab', 'plane'), may hold values from 0.2 to 1
- fibre_v: float32 [128, 2048], P('slab', 'plane'), may hold values from -4 to 4
- fibre_gates: float32 [40, 128, 2048], P(None, 'slab', 'plane'), may hold values from 0 to 1
- fibre_diff: float32 [128, 2048], P('slab', 'plane'), may hold values from 0.2 to 1
- gate_half: float32 [40], replicated, may hold values from -3 to 3
- gate_rate: float32 [40], replicated, may hold values from 0.5 to 20
- gate_cond: float32 [40], replicated, may hold values from 0.01 to 0.15
- gate_rev: float32 [40], replicated, may hold values from -2 to 2
- junc_cond: float32 [8], replicated, may hold values from 0.25 to 2
- junc_fibre: int32 [131072], P(('slab', 'plane')), may hold values from 0 to 15
- junc_fcell: int32 [131072], P(('slab', 'plane')), may hold values from 0 to 511
- junc_owner: int32 [131072, 1], P(('slab', 'plane')), may hold values from 0 to 31; in each aligned block of 4096 rows (0 to 4095, 4096 to 8191, ...) at most 256 rows name the same one
- junc_tcell: int32 [131072], P(('slab', 'plane')), may hold values from 0 to 8191
- junc_class: int32 [131072], P(('slab', 'plane')), may hold values from 0 to 7
Outputs:
- tissue_out: float32 [32, 64, 128], P('slab', 'plane')
- fibre_out: float32 [128, 2048], P('slab', 'plane')
The draws below stay inside these ranges and needn't reach their ends.
Inputs may be any that keep to these rules, and one draw needn't show every extreme that they name: `junc_owner`: among the junctions held by one device, no tissue block is named by more than 256 of them, and some block is named by exactly 256. `junc_fibre`: A fibre of the slab group of the device that holds the junction. `junc_fcell`: A cell of the holding device's share of that fibre. `junc_tcell`: numbered over the owner's block in the order z, y, x with x fastest.
All inputs are finite; a program needn't handle non-finite values.
Results may differ from the reference program's by a relative error of at most 0.00005.
Values sent between devices are 32-bit elements; how exact they have to be, the bound alone decides.
A program may use at most 64 MiB of HBM per device.

```python
import math
import jax
import jax.numpy as jnp
import numpy as np
from jax import lax

NX = 128
CY = 16
CZ = 4
FIB_DEV = 16
FCELLS = 2048
GATES = 40
CLASSES = 8
STEPS = 14
JUNC_DEV = 4096
CAP = 256
NZ = 32
NY = 64
NFIB = 128
JUNCS = 131072
N_PLANE = 4
DEVICES = 32


def set_ends(result, own_key, least, high):
    dims = result.shape
    index_at = [jax.random.randint(jax.random.fold_in(own_key, axis), (), 0, dims[axis]) for axis in range(len(dims))]
    result = result.at[tuple(index_at)].set(least)
    longest = dims.index(max(dims))
    index_at[longest] = (index_at[longest] + 1) % dims[longest]
    return result.at[tuple(index_at)].set(high)


def block_scale(rng, dims, pieces, smallest, largest):
    gain, own = 1.0, jax.random.fold_in(rng, 6)
    for axis_at, blocks in pieces:
        draws = jnp.exp(jax.random.uniform(jax.random.fold_in(own, axis_at), (blocks,), jnp.float32, smallest / len(pieces), largest / len(pieces)))
        gain = gain * jnp.repeat(draws, dims[axis_at] // blocks).reshape([-1 if axis == axis_at else 1 for axis in range(len(dims))])
    return gain


def shared_out(rng, own, number, rows, amount, top, reach, lean):
    ranking = jax.random.permutation(rng, amount)
    packed, usual = shares(amount, rows * top, reach, lean, True), shares(amount, rows * top, reach, lean, False)
    places = jnp.arange(amount)

    def named(sizes, rotation):
        used = int((sizes > 0).sum())
        fixed = max(1, used // 4)
        moved = fixed + (places - fixed + rotation * (used - fixed)) % max(1, amount - fixed)
        return jnp.zeros((amount,), jnp.int32).at[ranking[jnp.where(places < fixed, places, moved)]].set(jnp.asarray(sizes, jnp.int32))

    sizes = jnp.where(number % 4 == 0, named(packed, number // 4), named(usual, number - number // 4 - 1))
    mixed = jax.random.permutation(jax.random.fold_in(own, 3), amount)
    giver, sink = mixed[0:amount // 2 * 2:2], mixed[1:amount // 2 * 2:2]
    room = jnp.minimum(sizes[giver] - 1, reach - sizes[sink]) // 2
    room = jnp.where((giver == ranking[0]) | (sink == ranking[0]) | (sizes[sink] == 0), 0, jnp.maximum(room, 0))
    moved = jax.random.randint(jax.random.fold_in(own, 4), (amount // 2,), 0, 1 << 20) % (room + 1)
    sizes = sizes.at[giver].add(-moved).at[sink].add(moved)
    items = jnp.searchsorted(jnp.cumsum(sizes), jnp.arange(rows * top), side="right").astype(jnp.int32)
    table = items.reshape(top, rows).T
    table = table[jax.random.permutation(jax.random.fold_in(own, 1), rows)]
    rotation = jax.random.randint(jax.random.fold_in(own, 2), (rows, 1), 0, top)
    return jnp.take_along_axis(table, (jnp.arange(top)[None, :] + rotation) % top, axis=1)


def shares(count, total, limit, lean, full):
    loads = [(1 << 20) // math.isqrt(grade ** lean) + 1 for grade in range(1, count + 1)]
    largest = limit if full else min(limit, max(-(-total // count), total * loads[0] // sum(loads)))
    least = 1 if total - largest >= count - 1 else 0
    holding, surplus = [largest] + [least] * (count - 1), total - largest - least * (count - 1)
    while surplus > 0:
        candidates = [i for i in range(1, count) if holding[i] < largest] or [i for i in range(1, count) if holding[i] < limit]
        mass, remaining = sum([loads[i] for i in candidates]), surplus
        for i in candidates:
            extra = min(limit - holding[i], max(1, remaining * loads[i] // mass), surplus)
            holding[i] = holding[i] + extra
            surplus = surplus - extra
    return np.array(holding)


def centred(rng, shape, scale, bound, split=(), kind=jnp.bfloat16):
    drawn = jax.random.normal(rng, shape, jnp.float32) * scale
    if len(split) > 0:
        drawn = block_scale(rng, shape, split, -0.22, 0.18) * drawn
    return jnp.clip(drawn, min=-bound, max=bound).astype(kind)


def setup_inputs(seed: int = 0) -> dict:
    splits = jax.random.split(jax.random.key(seed), 17)
    tissue_v = centred(splits[0], (NZ, NY, NX), 1.0, 4.0, ((0, 8), (1, 4)), jnp.float32)
    tissue_gates = jnp.clip(1.0 * jax.random.uniform(splits[1], (GATES, NZ, NY, NX), jnp.float32) ** block_scale(splits[1], (GATES, NZ, NY, NX), ((1, 8), (2, 4)), -0.2, 0.2), 0.0, 1.0)
    tissue_diff = jnp.clip(jnp.exp(math.log(1.0) - 1.609438 * jax.random.uniform(splits[2], (NZ, NY, NX), jnp.float32) ** block_scale(splits[2], (NZ, NY, NX), ((0, 8), (1, 4)), -0.2, 0.2)), 0.2, 1.0)
    fibre_v = centred(splits[3], (NFIB, FCELLS), 1.0, 4.0, ((0, 8), (1, 4)), jnp.float32)
    fibre_gates = jnp.clip(1.0 * jax.random.uniform(splits[4], (GATES, NFIB, FCELLS), jnp.float32) ** block_scale(splits[4], (GATES, NFIB, FCELLS), ((1, 8), (2, 4)), -0.2, 0.2), 0.0, 1.0)
    fibre_diff = jnp.clip(jnp.exp(math.log(1.0) - 1.609438 * jax.random.uniform(splits[5], (NFIB, FCELLS), jnp.float32) ** block_scale(splits[5], (NFIB, FCELLS), ((0, 8), (1, 4)), -0.2, 0.2)), 0.2, 1.0)
    gate_half = centred(splits[6], (GATES,), 1.0, 3.0, (), jnp.float32)
    gate_rate = jnp.clip(jnp.exp(jax.random.uniform(splits[7], (GATES,), jnp.float32, math.log(0.5), math.log(20.0))), 0.5, 20.0)
    gate_cond = jnp.clip(jnp.exp(jax.random.uniform(splits[8], (GATES,), jnp.float32, math.log(0.01), math.log(0.15))), 0.01, 0.15)
    gate_rev = jnp.clip(jax.random.uniform(splits[9], (GATES,), jnp.float32, -2.0, 2.0), -2.0, 2.0)
    junc_cond = jnp.clip(jnp.exp(jax.random.uniform(splits[10], (CLASSES,), jnp.float32, math.log(0.25), math.log(2.0))), 0.25, 2.0)
    junc_fibre = set_ends(jax.random.randint(splits[11], (JUNCS,), 0, FIB_DEV), jax.random.fold_in(splits[11], 1), 0, FIB_DEV - 1).astype(jnp.int32)
    junc_fcell = set_ends(jax.random.randint(splits[12], (JUNCS,), 0, FCELLS // N_PLANE), jax.random.fold_in(splits[12], 1), 0, (FCELLS // N_PLANE) - 1).astype(jnp.int32)
    junc_owner_keys = jax.random.split(jax.random.fold_in(splits[13], 1), JUNCS // JUNC_DEV)
    junc_owner_turns = jax.random.permutation(jax.random.fold_in(splits[13], 3), JUNCS // JUNC_DEV)
    junc_owner = jax.vmap(lambda own, number: shared_out(jax.random.fold_in(splits[13], 2), own, number, JUNC_DEV, DEVICES, 1, CAP, 2))(junc_owner_keys, junc_owner_turns).reshape((JUNCS, 1))
    junc_tcell = set_ends(jax.random.randint(splits[14], (JUNCS,), 0, CZ * CY * NX), jax.random.fold_in(splits[14], 1), 0, (CZ * CY * NX) - 1).astype(jnp.int32)
    junc_class = set_ends(jax.random.randint(splits[15], (JUNCS,), 0, CLASSES), jax.random.fold_in(splits[15], 1), 0, CLASSES - 1).astype(jnp.int32)
    return {"tissue_v": tissue_v, "tissue_gates": tissue_gates, "tissue_diff": tissue_diff, "fibre_v": fibre_v, "fibre_gates": fibre_gates, "fibre_diff": fibre_diff, "gate_half": gate_half, "gate_rate": gate_rate, "gate_cond": gate_cond, "gate_rev": gate_rev, "junc_cond": junc_cond, "junc_fibre": junc_fibre, "junc_fcell": junc_fcell, "junc_owner": junc_owner, "junc_tcell": junc_tcell, "junc_class": junc_class}


time_step = 0.1
gate_slope = 2.0


def membrane(voltage, gates, gate_half, gate_rate, gate_cond, gate_rev):
    gate_signs = jnp.where(jnp.arange(GATES, dtype=jnp.int32) % 2 == 0, 1.0, -1.0).astype(jnp.float32)

    def one_gate(totals, inputs):
        gate_now, mid_point, speed, conductance, reversal, direction = inputs
        shifted = voltage - mid_point
        steady = jax.nn.sigmoid(direction * gate_slope * shifted)
        decay_factor = jnp.exp(-time_step * speed * (1.0 + jax.nn.sigmoid(shifted)))
        renewed = steady + (gate_now - steady) * decay_factor
        return (totals[0] + conductance * renewed, totals[1] + (conductance * reversal) * renewed), renewed

    zero_field = jnp.zeros_like(voltage)
    sums, renewed_all = lax.scan(one_gate, (zero_field, zero_field), (gates, gate_half, gate_rate, gate_cond, gate_rev, gate_signs))
    ionic = voltage * sums[0] - sums[1]
    return renewed_all, ionic


def line_count(length):
    places = jnp.arange(length, dtype=jnp.int32)
    return (places > 0).astype(jnp.float32) + (places < length - 1).astype(jnp.float32)


def reference(tissue_v, tissue_gates, tissue_diff, fibre_v, fibre_gates, fibre_diff, gate_half, gate_rate, gate_cond, gate_rev, junc_cond, junc_fibre, junc_fcell, junc_owner, junc_tcell, junc_class):
    depth_all, height_all, width_all = tissue_v.shape
    fibre_total, fibre_len = fibre_v.shape
    share = fibre_len // N_PLANE
    total_junctions = junc_fibre.shape[0]
    holder = jnp.arange(total_junctions, dtype=jnp.int32) // JUNC_DEV
    fibre_row = (holder // N_PLANE) * FIB_DEV + junc_fibre
    fibre_col = (holder % N_PLANE) * share + junc_fcell
    fibre_flat = (fibre_row * fibre_len + fibre_col).astype(jnp.int32)
    owners = junc_owner[:, 0]
    layer_z = (owners // N_PLANE) * CZ + junc_tcell // (CY * NX)
    row_y = (owners % N_PLANE) * CY + (junc_tcell // NX) % CY
    tissue_flat = ((layer_z * height_all + row_y) * width_all + junc_tcell % NX).astype(jnp.int32)
    coupling = jnp.sum(jnp.where(junc_class[:, None] == jnp.arange(CLASSES, dtype=jnp.int32)[None, :], junc_cond[None, :], jnp.zeros((), jnp.float32)), axis=1)
    tissue_count = line_count(depth_all)[:, None, None] + line_count(height_all)[None, :, None] + line_count(width_all)[None, None, :]
    fibre_count = line_count(fibre_len)[None, :]

    def advance(carry, unused):
        tissue_now, tissue_state, fibre_now, fibre_state = carry
        tissue_line = tissue_now.reshape(-1)
        fibre_line = fibre_now.reshape(-1)
        current = coupling * (fibre_line[fibre_flat] - tissue_line[tissue_flat])
        tissue_source = jnp.zeros_like(tissue_line).at[tissue_flat].add(current).reshape(tissue_now.shape)
        fibre_source = jnp.zeros_like(fibre_line).at[fibre_flat].add(-current).reshape(fibre_now.shape)
        padded = jnp.pad(tissue_now, 1)
        neighbours = padded[2:, 1:-1, 1:-1] + padded[:-2, 1:-1, 1:-1] + padded[1:-1, 2:, 1:-1] + padded[1:-1, :-2, 1:-1] + padded[1:-1, 1:-1, 2:] + padded[1:-1, 1:-1, :-2]
        tissue_lap = neighbours - tissue_count * tissue_now
        fibre_padded = jnp.pad(fibre_now, ((0, 0), (1, 1)))
        fibre_lap = fibre_padded[:, 2:] + fibre_padded[:, :-2] - fibre_count * fibre_now
        tissue_state, tissue_ionic = membrane(tissue_now, tissue_state, gate_half, gate_rate, gate_cond, gate_rev)
        fibre_state, fibre_ionic = membrane(fibre_now, fibre_state, gate_half, gate_rate, gate_cond, gate_rev)
        tissue_next = tissue_now + time_step * (tissue_diff * tissue_lap - tissue_ionic + tissue_source)
        fibre_next = fibre_now + time_step * (fibre_diff * fibre_lap - fibre_ionic + fibre_source)
        return (tissue_next, tissue_state, fibre_next, fibre_state), None

    final, unused_out = lax.scan(advance, (tissue_v, tissue_gates, fibre_v, fibre_gates), None, length=STEPS)
    return final[0], final[2]
```

```python
import functools
import math

import jax
import jax.numpy as jnp
from jax import lax
from jax.experimental import pallas as pl
from jax.experimental.pallas import tpu as pltpu
from jax.sharding import PartitionSpec as P

STEPS = 14
MESH = pl.DeviceIdType.MESH

time_step = 0.1
LANES = 128
SUBS = 8
WAVES = 4
UNROLL = 4


def class_gain(classes, junc_cond):
    return jnp.sum(
        jnp.where(
            classes[..., None] == jnp.arange(junc_cond.shape[0], dtype=jnp.int32),
            junc_cond,
            jnp.zeros((), jnp.float32),
        ),
        axis=-1,
    )


def make_onehot(indices, count):
    return (indices[:, None] == jnp.arange(count, dtype=jnp.int32)[None, :]).astype(jnp.float32)


def running_rank(owner_onehot):
    total, kinds = owner_onehot.shape
    tall = 128
    blocks = owner_onehot.astype(jnp.bfloat16).reshape(total // tall, tall, kinds)
    lower = jnp.tril(jnp.ones((tall, tall), jnp.bfloat16))
    within = jnp.einsum("ij,bjo->bio", lower, blocks, preferred_element_type=jnp.float32)
    sums = within[:, -1, :]
    count = total // tall
    before = jnp.tril(jnp.ones((count, count), jnp.float32), -1)
    ahead = jnp.dot(before, sums, precision=lax.Precision.HIGHEST)
    ranks = jnp.sum((within + ahead[:, None, :]).reshape(total, kinds) * owner_onehot, axis=1)
    return jnp.round(ranks).astype(jnp.int32) - 1


def place_values(row_onehot, col_onehot, values):
    weighted = col_onehot * values[:, None]
    return lax.dot_general(
        row_onehot,
        weighted,
        (((0,), (0,)), ((), ())),
        precision=lax.Precision.HIGHEST,
        preferred_element_type=jnp.float32,
    )


def flip_bits(value, bits):
    out, place = value, 1
    while place <= bits:
        if bits & place:
            out = out + place * (1 - 2 * ((value // place) % 2))
        place *= 2
    return out


def lane_gather(source, index):
    return lax.gather(
        source,
        index[..., None],
        lax.GatherDimensionNumbers(
            offset_dims=(),
            collapsed_slice_dims=(1,),
            start_index_map=(1,),
            operand_batching_dims=(0,),
            start_indices_batching_dims=(0,),
        ),
        slice_sizes=(1, 1),
        mode=lax.GatherScatterMode.PROMISE_IN_BOUNDS,
    )


def steps_kernel(
    sizes,
    coef,
    tissue_v,
    tissue_gates,
    tissue_diff,
    fibre_v,
    fibre_gates,
    fibre_diff,
    grow,
    gcol,
    hotrow,
    gain,
    colhot,
    tissue_out,
    fibre_out,
    volt,
    gate,
    pre,
    diff,
    rowhot,
    send,
    local,
    recv,
    zrecv,
    hsend,
    hrecv,
    send_sem,
    recv_sem,
    hsend_sem,
    hrecv_sem,
):
    slabs, planes, layers, yb, fb, cb, deep = sizes
    n = slabs * planes
    nt = layers * yb
    nq = nt + fb * cb
    gates = gate.shape[0]
    rows = SUBS * nt
    chunk = 2 * deep
    per = SUBS // chunk
    groups = n // per
    wave = n // WAVES
    slab = lax.axis_index("slab")
    plane = lax.axis_index("plane")

    def device(k):
        return (flip_bits(slab, k // planes), flip_bits(plane, k % planes))

    barrier = pltpu.get_barrier_semaphore()
    zero = jnp.zeros((SUBS, LANES), jnp.float32)
    for par in range(2):
        for way in range(2):
            for i in range(yb):
                zrecv[par, way, i] = zero
            for i in range(fb + 1):
                hrecv[par, way, i] = zero
    for way in range(2):
        hsend[way, fb] = zero
    for k in range(1, n):
        pl.semaphore_signal(barrier, inc=1, device_id=device(k), device_id_type=MESH)

    for z in range(layers):
        for y in range(yb):
            volt[z * yb + y] = tissue_v[z, SUBS * y : SUBS * (y + 1), :]
            diff[z * yb + y] = time_step * tissue_diff[z, SUBS * y : SUBS * (y + 1), :]
    for f in range(fb):
        for c in range(cb):
            at = (slice(SUBS * f, SUBS * (f + 1)), slice(LANES * c, LANES * (c + 1)))
            volt[nt + f * cb + c] = fibre_v[at]
            diff[nt + f * cb + c] = time_step * fibre_diff[at]

    @pl.loop(0, gates)
    def _(k):
        sign = coef[5, k]
        for z in range(layers):
            for y in range(yb):
                old = tissue_gates[k, z, SUBS * y : SUBS * (y + 1), :]
                gate[k, z * yb + y] = (old + old - 1.0) * sign
        for f in range(fb):
            for c in range(cb):
                old = fibre_gates[k, SUBS * f : SUBS * (f + 1), LANES * c : LANES * (c + 1)]
                gate[k, nt + f * cb + c] = (old + old - 1.0) * sign

    places = lax.broadcasted_iota(jnp.int32, (rows, LANES), 0)

    @pl.loop(0, n)
    def _(k):
        for i in range(chunk):
            hot = places == jnp.broadcast_to(hotrow[k, i : i + 1, :], (rows, LANES))
            rowhot[k, i] = jnp.where(hot, 1.0, 0.0).astype(jnp.bfloat16)

    pl.semaphore_wait(barrier, n - 1)

    sub = lax.broadcasted_iota(jnp.int32, (SUBS, LANES), 0)
    lane = lax.broadcasted_iota(jnp.int32, (SUBS, LANES), 1)
    is_fibre = sub % chunk < deep

    def gather_group(m):
        row_at = grow[m]
        col_at = gcol[m]
        out = zero
        for r in range(rows):
            q, s = r // SUBS, r % SUBS
            source = jnp.where(
                is_fibre,
                jnp.broadcast_to(volt[nt + q, s : s + 1, :], (SUBS, LANES)),
                jnp.broadcast_to(volt[q, s : s + 1, :], (SUBS, LANES)),
            )
            out = jnp.where(row_at == r, lane_gather(source, col_at), out)
        return out

    def junction_copy(k, par):
        return pltpu.make_async_remote_copy(
            src_ref=send.at[k],
            dst_ref=recv.at[par, k],
            send_sem=send_sem,
            recv_sem=recv_sem.at[par, k // wave],
            device_id=device(k),
            device_id_type=MESH,
        )

    def z_copy(way, par):
        first = (layers - 1) * yb if way == 0 else 0
        return pltpu.make_async_remote_copy(
            src_ref=volt.at[pl.ds(first, yb)],
            dst_ref=zrecv.at[par, way],
            send_sem=hsend_sem.at[way],
            recv_sem=hrecv_sem.at[par, way],
            device_id=(slab + 1 - 2 * way, plane),
            device_id_type=MESH,
        )

    def h_copy(way, par):
        return pltpu.make_async_remote_copy(
            src_ref=hsend.at[way],
            dst_ref=hrecv.at[par, way],
            send_sem=hsend_sem.at[2 + way],
            recv_sem=hrecv_sem.at[par, 2 + way],
            device_id=(slab, plane + 1 - 2 * way),
            device_id_type=MESH,
        )

    halos = (
        (z_copy, 0, slab < slabs - 1, slab > 0),
        (z_copy, 1, slab > 0, slab < slabs - 1),
        (h_copy, 0, plane < planes - 1, plane > 0),
        (h_copy, 1, plane > 0, plane < planes - 1),
    )

    def flag(condition):
        return jnp.where(condition, 1.0, 0.0)

    @pl.loop(0, STEPS)
    def _(step):
        par = step % 2
        for m in range(groups - 1, -1, -1):
            got = gather_group(m)
            if chunk == SUBS:
                swapped = pltpu.roll(got, deep, 0)
            else:
                swapped = jnp.where(
                    is_fibre, pltpu.roll(got, SUBS - deep, 0), pltpu.roll(got, deep, 0)
                )
            for p in range(per):
                send[per * m + p] = got[chunk * p : chunk * (p + 1)]
                local[per * m + p] = swapped[chunk * p : chunk * (p + 1)]
            if m < groups - 1:
                for p in range(per - 1, -1, -1):
                    junction_copy(per * (m + 1) + p, par).start()
        recv[par, 0] = send[0]
        for f in range(fb):
            hsend[0, f] = pltpu.roll(volt[nt + f * cb + cb - 1], 1, 1)
            hsend[1, f] = pltpu.roll(volt[nt + f * cb], LANES - 1, 1)
        for z in range(layers):
            hsend[0, fb, z : z + 1, :] = volt[z * yb + yb - 1, SUBS - 1 : SUBS, :]
            hsend[1, fb, z : z + 1, :] = volt[z * yb, 0:1, :]
        for p in range(per - 1, 0, -1):
            junction_copy(p, par).start()
        for build, way, sends, receives in halos:

            @pl.when(sends)
            def _():
                build(way, par).start()

        half_set = nq // 2
        for first in (0, half_set):

            @functools.partial(
                lax.fori_loop, 0, gates // UNROLL, init_val=(zero,) * (2 * half_set)
            )
            def sums(step_k, carry):
                carry = list(carry)
                for u in range(UNROLL):
                    k = step_k * UNROLL + u
                    half, base, slope, cond, pull = (coef[i, k] for i in range(5))
                    for i in range(half_set):
                        q = first + i
                        shifted = volt[q] - half
                        target = jnp.tanh(shifted)
                        factor = jnp.exp2(base + slope * jnp.tanh(0.5 * shifted))
                        new = target + (gate[k, q] - target) * factor
                        gate[k, q] = new
                        carry[2 * i] = carry[2 * i] + cond * new
                        carry[2 * i + 1] = carry[2 * i + 1] + pull * new
                return tuple(carry)

            for i in range(half_set):
                pre[first + i] = volt[first + i] * (coef[6, 0] + sums[2 * i]) - (
                    coef[6, 1] + sums[2 * i + 1]
                )

        at_left, at_right = lane == 0, lane == LANES - 1
        for z in range(layers):
            for y in range(yb):
                q = z * yb + y
                v = volt[q]
                near = jnp.where(at_left, 0.0, pltpu.roll(v, 1, 1))
                near = near + jnp.where(at_right, 0.0, pltpu.roll(v, LANES - 1, 1))
                above = pltpu.roll(volt[q - 1], 1, 0) if y > 0 else zero
                below = pltpu.roll(volt[q + 1], SUBS - 1, 0) if y < yb - 1 else zero
                near = near + jnp.where(sub == 0, above, pltpu.roll(v, 1, 0))
                near = near + jnp.where(sub == SUBS - 1, below, pltpu.roll(v, SUBS - 1, 0))
                count = jnp.where(at_left | at_right, 5.0, 6.0)
                if y == 0:
                    count = count - jnp.where(sub == 0, flag(plane == 0), 0.0)
                if y == yb - 1:
                    count = count - jnp.where(sub == SUBS - 1, flag(plane == planes - 1), 0.0)
                if z > 0:
                    near = near + volt[q - yb]
                else:
                    count = count - flag(slab == 0)
                if z < layers - 1:
                    near = near + volt[q + yb]
                else:
                    count = count - flag(slab == slabs - 1)
                pre[q] = v + diff[q] * (near - count * v) - time_step * pre[q]
        for f in range(fb):
            for c in range(cb):
                q = nt + f * cb + c
                v = volt[q]
                before = pltpu.roll(volt[q - 1], 1, 1) if c > 0 else zero
                after = pltpu.roll(volt[q + 1], LANES - 1, 1) if c < cb - 1 else zero
                near = jnp.where(at_left, before, pltpu.roll(v, 1, 1))
                near = near + jnp.where(at_right, after, pltpu.roll(v, LANES - 1, 1))
                count = jnp.full((SUBS, LANES), 2.0, jnp.float32)
                if c == 0:
                    count = count - jnp.where(at_left, flag(plane == 0), 0.0)
                if c == cb - 1:
                    count = count - jnp.where(at_right, flag(plane == planes - 1), 0.0)
                pre[q] = v + diff[q] * (near - count * v) - time_step * pre[q]

        sums = [jnp.zeros((2 * rows, LANES), jnp.float32) for _ in range(2)]
        for w in range(WAVES):
            span = pl.ds(w * wave + (1 if w == 0 else 0), wave - (1 if w == 0 else 0))
            pltpu.make_async_copy(
                recv.at[par, span], recv.at[par, span], recv_sem.at[par, w]
            ).wait()
            for k in range(w * wave, (w + 1) * wave):
                flow = gain[k] * (recv[par, k] - local[k])
                for kind in range(2):
                    parts = []
                    for i in range(kind * deep, (kind + 1) * deep):
                        value = jnp.broadcast_to(flow[i : i + 1, :], (2 * SUBS, LANES))
                        high = value.astype(jnp.bfloat16)
                        low = (value - high.astype(jnp.float32)).astype(jnp.bfloat16)
                        hot = rowhot[k, i]
                        tall = rows // (2 * SUBS)
                        parts.append(
                            jnp.concatenate(
                                [hot * jnp.concatenate([high] * tall, axis=0)]
                                + [hot * jnp.concatenate([low] * tall, axis=0)],
                                axis=0,
                            )
                        )
                    wide = jnp.concatenate(parts, axis=1) if deep > 1 else parts[0]
                    sums[kind] = sums[kind] + jnp.dot(
                        wide, colhot[k, kind], preferred_element_type=jnp.float32
                    )
        pltpu.make_async_copy(send.at[pl.ds(1, n - 1)], send.at[pl.ds(1, n - 1)], send_sem).wait()
        for build, way, sends, receives in halos:

            @pl.when(receives)
            def _():
                build(way, par).wait_recv()

            @pl.when(sends)
            def _():
                build(way, par).wait_send()

        new = []
        for z in range(layers):
            for y in range(yb):
                q = z * yb + y
                source = sums[0][SUBS * q : SUBS * (q + 1)]
                source = source + sums[0][rows + SUBS * q : rows + SUBS * (q + 1)]
                halo = zero
                if z == 0:
                    halo = halo + zrecv[par, 0, y]
                if z == layers - 1:
                    halo = halo + zrecv[par, 1, y]
                if y == 0:
                    row = jnp.broadcast_to(hrecv[par, 0, fb, z : z + 1, :], (SUBS, LANES))
                    halo = halo + jnp.where(sub == 0, row, 0.0)
                if y == yb - 1:
                    row = jnp.broadcast_to(hrecv[par, 1, fb, z : z + 1, :], (SUBS, LANES))
                    halo = halo + jnp.where(sub == SUBS - 1, row, 0.0)
                new.append(pre[q] + diff[q] * halo + time_step * source)
        for f in range(fb):
            for c in range(cb):
                q = f * cb + c
                source = sums[1][SUBS * q : SUBS * (q + 1)]
                source = source + sums[1][rows + SUBS * q : rows + SUBS * (q + 1)]
                halo = zero
                if c == 0:
                    halo = halo + jnp.where(at_left, hrecv[par, 0, f], 0.0)
                if c == cb - 1:
                    halo = halo + jnp.where(at_right, hrecv[par, 1, f], 0.0)
                new.append(pre[nt + q] + diff[nt + q] * halo + time_step * source)
        for q in range(nq):
            volt[q] = new[q]

    for z in range(layers):
        for y in range(yb):
            tissue_out[z, SUBS * y : SUBS * (y + 1), :] = volt[z * yb + y]
    for f in range(fb):
        for c in range(cb):
            at = (slice(SUBS * f, SUBS * (f + 1)), slice(LANES * c, LANES * (c + 1)))
            fibre_out[at] = volt[nt + f * cb + c]


def body(
    tissue_v,
    tissue_gates,
    tissue_diff,
    fibre_v,
    fibre_gates,
    fibre_diff,
    gate_half,
    gate_rate,
    gate_cond,
    gate_rev,
    junc_cond,
    junc_fibre,
    junc_fcell,
    junc_owner,
    junc_tcell,
    junc_class,
):
    slabs = lax.axis_size("slab")
    planes = lax.axis_size("plane")
    n = slabs * planes
    me = lax.axis_index("slab") * planes + lax.axis_index("plane")
    layers, rows_dev, cols_dev = tissue_v.shape
    fibre_rows, fibre_cols = fibre_v.shape
    junctions = junc_fibre.shape[0]
    capacity = 2 * junctions // n
    deep = -(-capacity // LANES)
    chunk = 2 * deep
    yb, fb, cb = rows_dev // SUBS, fibre_rows // SUBS, fibre_cols // LANES
    nt = layers * yb
    nq = nt + fb * cb
    rows = nt * SUBS
    owner_onehot = make_onehot(junc_owner[:, 0], n)
    rank_onehot = make_onehot(running_rank(owner_onehot), capacity)
    kinds = junc_cond.shape[0] + 1
    code = (junc_tcell * kinds + junc_class + 1).astype(jnp.float32)
    code_table = jnp.round(place_values(owner_onehot, rank_onehot, code)).astype(jnp.int32)
    fibre_index = (junc_fibre * fibre_cols + junc_fcell).astype(jnp.float32)
    own_cells = jnp.round(place_values(owner_onehot, rank_onehot, fibre_index)).astype(jnp.int32)
    sent = jnp.stack([code_table // kinds, code_table % kinds - 1])
    got = lax.all_to_all(sent, ("slab", "plane"), split_axis=1, concat_axis=1, tiled=True)
    near = me ^ jnp.arange(n, dtype=jnp.int32)
    full = jnp.stack([own_cells, sent[1], got[0], got[1]])
    full = jnp.take(full, near, axis=1)
    edge = deep * LANES - capacity
    full = jnp.pad(full, ((0, 0), (0, 0), (0, edge)), constant_values=-1)
    full = full.reshape(4, n, deep, LANES)
    own, own_class, cell, cell_class = full[0], full[1], full[2], full[3]
    own, cell = jnp.maximum(own, 0), jnp.maximum(cell, 0)
    fibre, along = own // fibre_cols, own % fibre_cols
    own_row = ((fibre // SUBS) * cb + along // LANES) * SUBS + fibre % SUBS
    own_col = along % LANES
    cell_row, cell_col = cell // LANES, cell % LANES
    grow = jnp.concatenate([own_row, cell_row], axis=1).reshape(-1, SUBS, LANES)
    gcol = jnp.concatenate([own_col, cell_col], axis=1).reshape(-1, SUBS, LANES)
    hotrow = jnp.concatenate([cell_row, own_row], axis=1)
    gain = class_gain(jnp.concatenate([cell_class, own_class], axis=1), junc_cond)
    cols = jnp.stack([cell_col, own_col], axis=1).reshape(n, 2, deep * LANES)
    colhot = (cols[..., None] == jnp.arange(LANES, dtype=jnp.int32)).astype(jnp.bfloat16)
    sign = jnp.where(jnp.arange(gate_half.shape[0]) % 2 == 0, 1.0, -1.0).astype(jnp.float32)
    rate = (-time_step * math.log2(math.e)) * gate_rate
    half_cond = 0.5 * gate_cond
    total = jnp.zeros_like(gate_half).at[0].set(jnp.sum(half_cond))
    total = total.at[1].set(jnp.sum(half_cond * gate_rev))
    coef = jnp.stack(
        [
            gate_half,
            1.5 * rate,
            0.5 * rate,
            sign * half_cond,
            sign * half_cond * gate_rev,
            sign,
            total,
        ]
    )
    vmem = pl.BlockSpec(memory_space=pltpu.VMEM)
    return pl.pallas_call(
        functools.partial(steps_kernel, (slabs, planes, layers, yb, fb, cb, deep)),
        out_shape=(
            jax.ShapeDtypeStruct(tissue_v.shape, jnp.float32),
            jax.ShapeDtypeStruct(fibre_v.shape, jnp.float32),
        ),
        in_specs=[pl.BlockSpec(memory_space=pltpu.SMEM)] + [vmem] * 11,
        out_specs=(vmem, vmem),
        scratch_shapes=[
            pltpu.VMEM((nq, SUBS, LANES), jnp.float32),
            pltpu.VMEM((gate_half.shape[0], nq, SUBS, LANES), jnp.float32),
            pltpu.VMEM((nq, SUBS, LANES), jnp.float32),
            pltpu.VMEM((nq, SUBS, LANES), jnp.float32),
            pltpu.VMEM((n, chunk, rows, LANES), jnp.bfloat16),
            pltpu.VMEM((n, chunk, LANES), jnp.float32),
            pltpu.VMEM((n, chunk, LANES), jnp.float32),
            pltpu.VMEM((2, n, chunk, LANES), jnp.float32),
            pltpu.VMEM((2, 2, yb, SUBS, LANES), jnp.float32),
            pltpu.VMEM((2, fb + 1, SUBS, LANES), jnp.float32),
            pltpu.VMEM((2, 2, fb + 1, SUBS, LANES), jnp.float32),
            pltpu.SemaphoreType.DMA,
            pltpu.SemaphoreType.DMA((2, WAVES)),
            pltpu.SemaphoreType.DMA((4,)),
            pltpu.SemaphoreType.DMA((2, 4)),
        ],
        compiler_params=pltpu.CompilerParams(
            collective_id=0, has_side_effects=True, vmem_limit_bytes=58 * 1024 * 1024
        ),
    )(
        coef,
        tissue_v,
        tissue_gates,
        tissue_diff,
        fibre_v,
        fibre_gates,
        fibre_diff,
        grow,
        gcol,
        hotrow,
        gain,
        colhot,
    )


def solution(mesh):
    in_specs = (
        P("slab", "plane", None),
        P(None, "slab", "plane", None),
        P("slab", "plane", None),
        P("slab", "plane"),
        P(None, "slab", "plane"),
        P("slab", "plane"),
        P(),
        P(),
        P(),
        P(),
        P(),
        P(("slab", "plane")),
        P(("slab", "plane")),
        P(("slab", "plane"), None),
        P(("slab", "plane")),
        P(("slab", "plane")),
    )
    out_specs = (P("slab", "plane", None), P("slab", "plane"))
    return jax.shard_map(body, mesh=mesh, in_specs=in_specs, out_specs=out_specs, check_vma=False)
```

```python
import functools
import math

import jax
import jax.numpy as jnp
from jax import lax
from jax.experimental import pallas as pl
from jax.experimental.pallas import tpu as pltpu
from jax.sharding import PartitionSpec as P

STEPS = 14
MESH = pl.DeviceIdType.MESH

time_step = 0.1
LANES = 128
SUBS = 8
WAVES = 4
UNROLL = 4


def flip_bits(value, bits):
    out, place = value, 1
    while place <= bits:
        if bits & place:
            out = out + place * (1 - 2 * ((value // place) % 2))
        place *= 2
    return out


def axis_gather(source, index, axis):
    other = 1 - axis
    return lax.gather(
        source,
        index[..., None],
        lax.GatherDimensionNumbers(
            offset_dims=(),
            collapsed_slice_dims=(axis,),
            start_index_map=(axis,),
            operand_batching_dims=(other,),
            start_indices_batching_dims=(other,),
        ),
        slice_sizes=(1, 1),
        mode=lax.GatherScatterMode.PROMISE_IN_BOUNDS,
    )


def swap_partner(tiles, bit, sub_bits, lane_bits):
    sub = lax.broadcasted_iota(jnp.int32, (SUBS, LANES), 0)
    lane = lax.broadcasted_iota(jnp.int32, (SUBS, LANES), 1)
    if bit < sub_bits:
        return [tiles[v ^ (1 << bit)] for v in range(len(tiles))]
    if bit < lane_bits:
        axis, place, size, reach = 0, sub, SUBS, 1 << (bit - sub_bits)
    else:
        axis, place, size, reach = 1, lane, LANES, 1 << (bit - lane_bits)
    if 2 * reach == size:
        return [pltpu.roll(tile, reach, axis) for tile in tiles]
    low = (place & reach) == 0
    return [
        jnp.where(low, pltpu.roll(tile, size - reach, axis), pltpu.roll(tile, reach, axis))
        for tile in tiles
    ]


def sort_tiles(tiles):
    sub = lax.broadcasted_iota(jnp.int32, (SUBS, LANES), 0)
    lane = lax.broadcasted_iota(jnp.int32, (SUBS, LANES), 1)
    sub_bits = (len(tiles) - 1).bit_length()
    lane_bits = sub_bits + 3
    bits = lane_bits + 7
    spot = [v + (sub << sub_bits) + (lane << lane_bits) for v in range(len(tiles))]
    for size in range(1, bits + 1):
        for bit in range(size - 1, -1, -1):
            others = swap_partner(tiles, bit, sub_bits, lane_bits)
            new = []
            for at, tile, other in zip(spot, tiles, others):
                turn = (at >> bit) if size == bits else (at >> bit) ^ (at >> size)
                new.append(
                    jnp.where(
                        (turn & 1) == 0, jnp.minimum(tile, other), jnp.maximum(tile, other)
                    )
                )
            tiles = new
    return tiles


def steps_kernel(
    sizes,
    half_ref,
    rate_ref,
    cond_ref,
    rev_ref,
    class_ref,
    tissue_v,
    tissue_gates,
    tissue_diff,
    fibre_v,
    fibre_gates,
    fibre_diff,
    junc_owner,
    junc_fibre,
    junc_fcell,
    junc_tcell,
    junc_class,
    out_ref,
    volt,
    gate,
    pre,
    diff,
    rowhot,
    colhot,
    send,
    local,
    recv,
    zrecv,
    hsend,
    hrecv,
    coef,
    tissue_in,
    fibre_in,
    pad_a,
    pad_b,
    payload,
    dense,
    spread,
    hotrow,
    hotcol,
    gain,
    remote,
    sent_codes,
    got_codes,
    send_sem,
    recv_sem,
    hsend_sem,
    hrecv_sem,
    gate_sem,
    code_sems,
):
    slabs, planes, layers, yb, fb, cb, deep = sizes
    n = slabs * planes
    nt = layers * yb
    nq = nt + fb * cb
    gates = gate.shape[0]
    rows = SUBS * nt
    chunk = 2 * deep
    per = SUBS // deep
    groups = n // per
    wave = n // WAVES
    slab = lax.axis_index("slab")
    plane = lax.axis_index("plane")

    def device(k):
        return (flip_bits(slab, k // planes), flip_bits(plane, k % planes))

    loads = [
        pltpu.make_async_copy(tissue_gates, tissue_in, gate_sem.at[0]),
        pltpu.make_async_copy(fibre_gates, fibre_in, gate_sem.at[1]),
    ]
    for load in loads:
        load.start()
    barrier = pltpu.get_barrier_semaphore()
    zero = jnp.zeros((SUBS, LANES), jnp.float32)
    for par in range(2):
        for way in range(2):
            for i in range(yb):
                zrecv[par, way, i] = zero
            for i in range(fb + 1):
                hrecv[par, way, i] = zero
    for way in range(2):
        hsend[way, fb] = zero
    for k in range(1, n):
        pl.semaphore_signal(barrier, inc=1, device_id=device(k), device_id_type=MESH)

    for z in range(layers):
        for y in range(yb):
            volt[z * yb + y] = tissue_v[z, SUBS * y : SUBS * (y + 1), :]
            diff[z * yb + y] = time_step * tissue_diff[z, SUBS * y : SUBS * (y + 1), :]
    for f in range(fb):
        for c in range(cb):
            at = (slice(SUBS * f, SUBS * (f + 1)), slice(LANES * c, LANES * (c + 1)))
            volt[nt + f * cb + c] = fibre_v[at]
            diff[nt + f * cb + c] = time_step * fibre_diff[at]

    sub = lax.broadcasted_iota(jnp.int32, (SUBS, LANES), 0)
    lane = lax.broadcasted_iota(jnp.int32, (SUBS, LANES), 1)
    me = slab * planes + plane
    classes = class_ref.shape[0]
    codes = rows * LANES * classes
    lines = junc_owner.shape[0]
    blocks = lines // SUBS
    total = lines * LANES
    tiles = []
    for v in range(blocks):
        at = slice(SUBS * v, SUBS * (v + 1))
        fibre, along = junc_fibre[at], junc_fcell[at]
        row = (fibre // SUBS * cb + along // LANES) * SUBS + fibre % SUBS
        code = junc_tcell[at] * classes + junc_class[at]
        payload[at] = (row * LANES + along % LANES) * codes + code
        tiles.append((junc_owner[at] ^ me) * total + (v * SUBS + sub) * LANES + lane)
    tiles = sort_tiles(tiles)
    for v in range(blocks):
        pad_a[pl.ds(v, SUBS, stride=blocks), :] = tiles[v]
    pad_b[:, 0:lines] = pad_a[...].T
    fold = LANES // lines
    lined = None
    wide_lane = lax.broadcasted_iota(jnp.int32, (lines, LANES), 1)
    for i in range(fold):
        piece = pad_b[pl.ds(i, lines, stride=fold), :]
        piece = pltpu.roll(piece, lines * i, 1) if i > 0 else piece
        lined = piece if i == 0 else jnp.where(wide_lane >= lines * i, piece, lined)
    facts = []
    for v in range(blocks):
        key = lined[SUBS * v : SUBS * (v + 1)]
        spot = key % total
        fact = jnp.zeros((SUBS, LANES), jnp.int32)
        for r in range(lines):
            line = jnp.broadcast_to(payload[r : r + 1, :], (SUBS, LANES))
            fact = jnp.where(spot // LANES == r, axis_gather(line, spot % LANES, 1), fact)
        dense[v, 0] = fact // codes // LANES
        dense[v, 1] = fact // codes % LANES
        facts.append((key // total, (v * SUBS + sub + 1) * (2 * codes) + fact % codes + 1))
    for k in range(n):
        found = jnp.zeros((SUBS, LANES), jnp.int32)
        for owner, fact in facts:
            found = found + jnp.where(owner == k, fact, 0)
        reach = deep
        while reach < SUBS:
            found = found + pltpu.roll(found, reach, 0)
            reach *= 2
        sent_codes[k] = found[:deep] % (2 * codes)
        spread[k] = jnp.maximum(found[:deep] // (2 * codes) - 1, 0)
    got_codes[0] = sent_codes[0]

    pl.semaphore_wait(barrier, n - 1)
    for k in range(n - 1, 0, -1):
        pltpu.make_async_remote_copy(
            src_ref=sent_codes.at[k],
            dst_ref=got_codes.at[k],
            send_sem=code_sems.at[0],
            recv_sem=code_sems.at[1],
            device_id=device(k),
            device_id_type=MESH,
        ).start()

    def set_coef(k, carry):
        even = jnp.where(k % 2 == 0, 1.0, -1.0)
        half_cond = 0.5 * cond_ref[k]
        scaled = (-time_step * math.log2(math.e)) * rate_ref[k]
        coef[0, k] = half_ref[k]
        coef[1, k] = 1.5 * scaled
        coef[2, k] = 0.5 * scaled
        coef[3, k] = even * half_cond
        coef[4, k] = even * half_cond * rev_ref[k]
        coef[5, k] = even
        return carry[0] + half_cond, carry[1] + half_cond * rev_ref[k]

    zero_scalar = jnp.float32(0.0)
    sum_cond, sum_pull = lax.fori_loop(0, gates, set_coef, (zero_scalar, zero_scalar))

    places = lax.broadcasted_iota(jnp.int32, (rows, LANES), 0)
    columns = lax.broadcasted_iota(jnp.int32, (LANES, LANES), 0)

    def set_hot(k, kind, i, row, col):
        hot = places == jnp.broadcast_to(row, (rows, LANES))
        rowhot[k, kind * deep + i] = jnp.where(hot, 1.0, 0.0).astype(jnp.bfloat16)
        hot = columns == jnp.broadcast_to(col, (LANES, LANES))
        hot = jnp.where(hot, 1.0, 0.0).astype(jnp.bfloat16)
        colhot[k, kind, LANES * i : LANES * (i + 1), :] = hot.T

    def gain_of(code):
        kind = code % classes
        out = jnp.zeros(code.shape, jnp.float32)
        for c in range(classes):
            out = jnp.where(kind == c, class_ref[c], out)
        return out

    def tall_tile(value):
        return jnp.concatenate([value] * (SUBS // deep), axis=0) if deep < SUBS else value

    @pl.loop(0, n)
    def _(k):
        spot = tall_tile(spread[k])
        row = jnp.zeros((SUBS, LANES), jnp.int32)
        col = row
        for v in range(blocks):
            here = spot // SUBS == v
            row = jnp.where(here, axis_gather(dense[v, 0], spot % SUBS, 0), row)
            col = jnp.where(here, axis_gather(dense[v, 1], spot % SUBS, 0), col)
        code = sent_codes[k]
        gain[k, deep:chunk] = jnp.where(code > 0, gain_of(code - 1), 0.0)
        for i in range(deep):
            set_hot(k, 1, i, row[i : i + 1], col[i : i + 1])

    for load in loads:
        load.wait()

    @pl.loop(0, gates)
    def _(k):
        sign = coef[5, k]
        for z in range(layers):
            for y in range(yb):
                old = tissue_in[k, z, SUBS * y : SUBS * (y + 1), :]
                gate[k, z * yb + y] = (old + old - 1.0) * sign
        for f in range(fb):
            for c in range(cb):
                old = fibre_in[k, SUBS * f : SUBS * (f + 1), LANES * c : LANES * (c + 1)]
                gate[k, nt + f * cb + c] = (old + old - 1.0) * sign

    far = pl.ds(1, n - 1)
    pltpu.make_async_copy(got_codes.at[far], got_codes.at[far], code_sems.at[1]).wait()
    pltpu.make_async_copy(sent_codes.at[far], sent_codes.at[far], code_sems.at[0]).wait()

    @pl.loop(0, n)
    def _(k):
        code = got_codes[k]
        cell = jnp.maximum(code - 1, 0) // classes
        gain[k, 0:deep] = jnp.where(code > 0, gain_of(code - 1), 0.0)
        remote[0, k] = cell // LANES
        remote[1, k] = cell % LANES
        for i in range(deep):
            set_hot(k, 0, i, cell[i : i + 1] // LANES, cell[i : i + 1] % LANES)

    for m in range(n * deep // SUBS):
        for kind in range(2):
            parts = [remote[kind, m * (SUBS // deep) + p] for p in range(SUBS // deep)]
            hotrow[kind, m] = jnp.concatenate(parts, axis=0) if len(parts) > 1 else parts[0]
        parts = [spread[m * (SUBS // deep) + p] for p in range(SUBS // deep)]
        hotcol[m] = jnp.concatenate(parts, axis=0) if len(parts) > 1 else parts[0]

    def lookup(base, row_at, col_at):
        out = zero
        for r in range(rows):
            line = volt[base + r // SUBS, r % SUBS : r % SUBS + 1, :]
            line = jnp.broadcast_to(line, (SUBS, LANES))
            out = jnp.where(row_at == r, axis_gather(line, col_at, 1), out)
        return out

    def junction_copy(k, par):
        return pltpu.make_async_remote_copy(
            src_ref=send.at[k],
            dst_ref=recv.at[par, k],
            send_sem=send_sem,
            recv_sem=recv_sem.at[par, k // wave],
            device_id=device(k),
            device_id_type=MESH,
        )

    def z_copy(way, par):
        first = (layers - 1) * yb if way == 0 else 0
        return pltpu.make_async_remote_copy(
            src_ref=volt.at[pl.ds(first, yb)],
            dst_ref=zrecv.at[par, way],
            send_sem=hsend_sem.at[way],
            recv_sem=hrecv_sem.at[par, way],
            device_id=(slab + 1 - 2 * way, plane),
            device_id_type=MESH,
        )

    def h_copy(way, par):
        return pltpu.make_async_remote_copy(
            src_ref=hsend.at[way],
            dst_ref=hrecv.at[par, way],
            send_sem=hsend_sem.at[2 + way],
            recv_sem=hrecv_sem.at[par, 2 + way],
            device_id=(slab, plane + 1 - 2 * way),
            device_id_type=MESH,
        )

    halos = (
        (z_copy, 0, slab < slabs - 1, slab > 0),
        (z_copy, 1, slab > 0, slab < slabs - 1),
        (h_copy, 0, plane < planes - 1, plane > 0),
        (h_copy, 1, plane > 0, plane < planes - 1),
    )

    def flag(condition):
        return jnp.where(condition, 1.0, 0.0)

    @pl.loop(0, STEPS)
    def _(step):
        par = step % 2
        own = [lookup(nt, dense[v, 0], dense[v, 1]) for v in range(blocks)]
        for m in range(groups - 1, -1, -1):
            tissue_part = lookup(0, hotrow[0, m], hotrow[1, m])
            spot = hotcol[m]
            fibre_part = zero
            for v in range(blocks):
                fibre_part = jnp.where(
                    spot // SUBS == v, axis_gather(own[v], spot % SUBS, 0), fibre_part
                )
            for p in range(per):
                at = slice(deep * p, deep * (p + 1))
                k = per * m + p
                send[k, 0:deep] = fibre_part[at]
                send[k, deep:chunk] = tissue_part[at]
                local[k, 0:deep] = tissue_part[at]
                local[k, deep:chunk] = fibre_part[at]
            if m < groups - 1:
                for p in range(per - 1, -1, -1):
                    junction_copy(per * (m + 1) + p, par).start()
        recv[par, 0] = send[0]
        for f in range(fb):
            hsend[0, f] = pltpu.roll(volt[nt + f * cb + cb - 1], 1, 1)
            hsend[1, f] = pltpu.roll(volt[nt + f * cb], LANES - 1, 1)
        for z in range(layers):
            hsend[0, fb, z : z + 1, :] = volt[z * yb + yb - 1, SUBS - 1 : SUBS, :]
            hsend[1, fb, z : z + 1, :] = volt[z * yb, 0:1, :]
        for p in range(per - 1, 0, -1):
            junction_copy(p, par).start()
        for build, way, sends, receives in halos:

            @pl.when(sends)
            def _():
                build(way, par).start()

        half_set = nq // 2
        for first in (0, half_set):

            @functools.partial(
                lax.fori_loop, 0, gates // UNROLL, init_val=(zero,) * (2 * half_set)
            )
            def sums(step_k, carry):
                carry = list(carry)
                for u in range(UNROLL):
                    k = step_k * UNROLL + u
                    half, base, slope, cond, pull = (coef[i, k] for i in range(5))
                    for i in range(half_set):
                        q = first + i
                        shifted = volt[q] - half
                        target = jnp.tanh(shifted)
                        factor = jnp.exp2(base + slope * jnp.tanh(0.5 * shifted))
                        new = target + (gate[k, q] - target) * factor
                        gate[k, q] = new
                        carry[2 * i] = carry[2 * i] + cond * new
                        carry[2 * i + 1] = carry[2 * i + 1] + pull * new
                return tuple(carry)

            for i in range(half_set):
                pre[first + i] = volt[first + i] * (sum_cond + sums[2 * i]) - (
                    sum_pull + sums[2 * i + 1]
                )

        at_left, at_right = lane == 0, lane == LANES - 1
        for z in range(layers):
            for y in range(yb):
                q = z * yb + y
                v = volt[q]
                near = jnp.where(at_left, 0.0, pltpu.roll(v, 1, 1))
                near = near + jnp.where(at_right, 0.0, pltpu.roll(v, LANES - 1, 1))
                above = pltpu.roll(volt[q - 1], 1, 0) if y > 0 else zero
                below = pltpu.roll(volt[q + 1], SUBS - 1, 0) if y < yb - 1 else zero
                near = near + jnp.where(sub == 0, above, pltpu.roll(v, 1, 0))
                near = near + jnp.where(sub == SUBS - 1, below, pltpu.roll(v, SUBS - 1, 0))
                count = jnp.where(at_left | at_right, 5.0, 6.0)
                if y == 0:
                    count = count - jnp.where(sub == 0, flag(plane == 0), 0.0)
                if y == yb - 1:
                    count = count - jnp.where(sub == SUBS - 1, flag(plane == planes - 1), 0.0)
                if z > 0:
                    near = near + volt[q - yb]
                else:
                    count = count - flag(slab == 0)
                if z < layers - 1:
                    near = near + volt[q + yb]
                else:
                    count = count - flag(slab == slabs - 1)
                pre[q] = v + diff[q] * (near - count * v) - time_step * pre[q]
        for f in range(fb):
            for c in range(cb):
                q = nt + f * cb + c
                v = volt[q]
                before = pltpu.roll(volt[q - 1], 1, 1) if c > 0 else zero
                after = pltpu.roll(volt[q + 1], LANES - 1, 1) if c < cb - 1 else zero
                near = jnp.where(at_left, before, pltpu.roll(v, 1, 1))
                near = near + jnp.where(at_right, after, pltpu.roll(v, LANES - 1, 1))
                count = jnp.full((SUBS, LANES), 2.0, jnp.float32)
                if c == 0:
                    count = count - jnp.where(at_left, flag(plane == 0), 0.0)
                if c == cb - 1:
                    count = count - jnp.where(at_right, flag(plane == planes - 1), 0.0)
                pre[q] = v + diff[q] * (near - count * v) - time_step * pre[q]

        sums = [jnp.zeros((2 * rows, LANES), jnp.float32) for _ in range(2)]
        for w in range(WAVES):
            span = pl.ds(w * wave + (1 if w == 0 else 0), wave - (1 if w == 0 else 0))
            pltpu.make_async_copy(
                recv.at[par, span], recv.at[par, span], recv_sem.at[par, w]
            ).wait()
            for kind in range(2):
                for k in range(w * wave, (w + 1) * wave):
                    flow = gain[k] * (recv[par, k] - local[k])
                    parts = []
                    for i in range(kind * deep, (kind + 1) * deep):
                        value = jnp.broadcast_to(flow[i : i + 1, :], (2 * SUBS, LANES))
                        high = value.astype(jnp.bfloat16)
                        low = (value - high.astype(jnp.float32)).astype(jnp.bfloat16)
                        hot = rowhot[k, i]
                        tall = rows // (2 * SUBS)
                        parts.append(
                            jnp.concatenate(
                                [jnp.concatenate([high] * tall, axis=0) * hot]
                                + [jnp.concatenate([low] * tall, axis=0) * hot],
                                axis=0,
                            )
                        )
                    wide = jnp.concatenate(parts, axis=1) if deep > 1 else parts[0]
                    sums[kind] = sums[kind] + jnp.dot(
                        wide, colhot[k, kind], preferred_element_type=jnp.float32
                    )
        pltpu.make_async_copy(send.at[pl.ds(1, n - 1)], send.at[pl.ds(1, n - 1)], send_sem).wait()
        for build, way, sends, receives in halos:

            @pl.when(receives)
            def _():
                build(way, par).wait_recv()

            @pl.when(sends)
            def _():
                build(way, par).wait_send()

        new = []
        for z in range(layers):
            for y in range(yb):
                q = z * yb + y
                source = sums[0][SUBS * q : SUBS * (q + 1)]
                source = source + sums[0][rows + SUBS * q : rows + SUBS * (q + 1)]
                halo = zero
                if z == 0:
                    halo = halo + zrecv[par, 0, y]
                if z == layers - 1:
                    halo = halo + zrecv[par, 1, y]
                if y == 0:
                    row = jnp.broadcast_to(hrecv[par, 0, fb, z : z + 1, :], (SUBS, LANES))
                    halo = halo + jnp.where(sub == 0, row, 0.0)
                if y == yb - 1:
                    row = jnp.broadcast_to(hrecv[par, 1, fb, z : z + 1, :], (SUBS, LANES))
                    halo = halo + jnp.where(sub == SUBS - 1, row, 0.0)
                new.append(pre[q] + diff[q] * halo + time_step * source)
        for f in range(fb):
            for c in range(cb):
                q = f * cb + c
                source = sums[1][SUBS * q : SUBS * (q + 1)]
                source = source + sums[1][rows + SUBS * q : rows + SUBS * (q + 1)]
                halo = zero
                if c == 0:
                    halo = halo + jnp.where(at_left, hrecv[par, 0, f], 0.0)
                if c == cb - 1:
                    halo = halo + jnp.where(at_right, hrecv[par, 1, f], 0.0)
                new.append(pre[nt + q] + diff[nt + q] * halo + time_step * source)
        for q in range(nq):
            volt[q] = new[q]

    out_ref[...] = volt[...]


def body(
    tissue_v,
    tissue_gates,
    tissue_diff,
    fibre_v,
    fibre_gates,
    fibre_diff,
    gate_half,
    gate_rate,
    gate_cond,
    gate_rev,
    junc_cond,
    junc_fibre,
    junc_fcell,
    junc_owner,
    junc_tcell,
    junc_class,
):
    slabs = lax.axis_size("slab")
    planes = lax.axis_size("plane")
    n = slabs * planes
    layers, rows_dev, cols_dev = tissue_v.shape
    fibre_rows, fibre_cols = fibre_v.shape
    junctions = junc_fibre.shape[0]
    capacity = 2 * junctions // n
    deep = -(-capacity // LANES)
    chunk = 2 * deep
    yb, fb, cb = rows_dev // SUBS, fibre_rows // SUBS, fibre_cols // LANES
    nt = layers * yb
    nq = nt + fb * cb
    rows = nt * SUBS
    lines = junctions // LANES
    gates = gate_half.shape[0]
    per = SUBS // deep
    smem = pl.BlockSpec(memory_space=pltpu.SMEM)
    hbm = pl.BlockSpec(memory_space=pl.ANY)
    vmem = pl.BlockSpec(memory_space=pltpu.VMEM)
    flat = [
        x.reshape(lines, LANES) for x in (junc_owner, junc_fibre, junc_fcell, junc_tcell, junc_class)
    ]
    out = pl.pallas_call(
        functools.partial(steps_kernel, (slabs, planes, layers, yb, fb, cb, deep)),
        out_shape=jax.ShapeDtypeStruct((nq, SUBS, LANES), jnp.float32),
        in_specs=[smem] * 5 + [vmem, hbm, vmem, vmem, hbm, vmem] + [vmem] * 5,
        out_specs=vmem,
        scratch_shapes=[
            pltpu.VMEM((nq, SUBS, LANES), jnp.float32),
            pltpu.VMEM((gates, nq, SUBS, LANES), jnp.float32),
            pltpu.VMEM((nq, SUBS, LANES), jnp.float32),
            pltpu.VMEM((nq, SUBS, LANES), jnp.float32),
            pltpu.VMEM((n, chunk, rows, LANES), jnp.bfloat16),
            pltpu.VMEM((n, 2, deep * LANES, LANES), jnp.bfloat16),
            pltpu.VMEM((n, chunk, LANES), jnp.float32),
            pltpu.VMEM((n, chunk, LANES), jnp.float32),
            pltpu.VMEM((2, n, chunk, LANES), jnp.float32),
            pltpu.VMEM((2, 2, yb, SUBS, LANES), jnp.float32),
            pltpu.VMEM((2, fb + 1, SUBS, LANES), jnp.float32),
            pltpu.VMEM((2, 2, fb + 1, SUBS, LANES), jnp.float32),
            pltpu.SMEM((6, gates), jnp.float32),
            pltpu.VMEM(tissue_gates.shape, jnp.float32),
            pltpu.VMEM(fibre_gates.shape, jnp.float32),
            pltpu.VMEM((lines, LANES), jnp.int32),
            pltpu.VMEM((LANES, LANES), jnp.int32),
            pltpu.VMEM((lines, LANES), jnp.int32),
            pltpu.VMEM((lines // SUBS, 2, SUBS, LANES), jnp.int32),
            pltpu.VMEM((n, deep, LANES), jnp.int32),
            pltpu.VMEM((2, n // per, SUBS, LANES), jnp.int32),
            pltpu.VMEM((n // per, SUBS, LANES), jnp.int32),
            pltpu.VMEM((n, chunk, LANES), jnp.float32),
            pltpu.VMEM((2, n, deep, LANES), jnp.int32),
            pltpu.VMEM((n, deep, LANES), jnp.int32),
            pltpu.VMEM((n, deep, LANES), jnp.int32),
            pltpu.SemaphoreType.DMA,
            pltpu.SemaphoreType.DMA((2, WAVES)),
            pltpu.SemaphoreType.DMA((4,)),
            pltpu.SemaphoreType.DMA((2, 4)),
            pltpu.SemaphoreType.DMA((2,)),
            pltpu.SemaphoreType.DMA((2,)),
        ],
        compiler_params=pltpu.CompilerParams(
            collective_id=0, has_side_effects=True, vmem_limit_bytes=58 * 1024 * 1024
        ),
    )(
        gate_half,
        gate_rate,
        gate_cond,
        gate_rev,
        junc_cond,
        tissue_v,
        tissue_gates,
        tissue_diff,
        fibre_v,
        fibre_gates,
        fibre_diff,
        *flat,
    )
    fibre_out = out[nt:].reshape(fb, cb, SUBS, LANES).transpose(0, 2, 1, 3)
    return out[:nt].reshape(tissue_v.shape), fibre_out.reshape(fibre_v.shape)


def solution(mesh):
    in_specs = (
        P("slab", "plane", None),
        P(None, "slab", "plane", None),
        P("slab", "plane", None),
        P("slab", "plane"),
        P(None, "slab", "plane"),
        P("slab", "plane"),
        P(),
        P(),
        P(),
        P(),
        P(),
        P(("slab", "plane")),
        P(("slab", "plane")),
        P(("slab", "plane"), None),
        P(("slab", "plane")),
        P(("slab", "plane")),
    )
    out_specs = (P("slab", "plane", None), P("slab", "plane"))
    return jax.shard_map(body, mesh=mesh, in_specs=in_specs, out_specs=out_specs, check_vma=False)
```

```python
import functools
import math

import jax
import jax.numpy as jnp
from jax import lax
from jax.experimental import pallas as pl
from jax.experimental.pallas import tpu as pltpu
from jax.sharding import PartitionSpec as P

STEPS = 14
MESH = pl.DeviceIdType.MESH

time_step = 0.1
LANES = 128
SUBS = 8
WAVES = 4
UNROLL = 4


def flip_bits(value, bits):
    out, place = value, 1
    while place <= bits:
        if bits & place:
            out = out + place * (1 - 2 * ((value // place) % 2))
        place *= 2
    return out


def axis_gather(source, index, axis):
    other = 1 - axis
    return lax.gather(
        source,
        index[..., None],
        lax.GatherDimensionNumbers(
            offset_dims=(),
            collapsed_slice_dims=(axis,),
            start_index_map=(axis,),
            operand_batching_dims=(other,),
            start_indices_batching_dims=(other,),
        ),
        slice_sizes=(1, 1),
        mode=lax.GatherScatterMode.PROMISE_IN_BOUNDS,
    )


def swap_partner(tiles, bit, sub_bits, lane_bits):
    sub = lax.broadcasted_iota(jnp.int32, (SUBS, LANES), 0)
    lane = lax.broadcasted_iota(jnp.int32, (SUBS, LANES), 1)
    if bit < sub_bits:
        return [tiles[v ^ (1 << bit)] for v in range(len(tiles))]
    if bit < lane_bits:
        axis, place, size, reach = 0, sub, SUBS, 1 << (bit - sub_bits)
    else:
        axis, place, size, reach = 1, lane, LANES, 1 << (bit - lane_bits)
    if 2 * reach == size:
        return [pltpu.roll(tile, reach, axis) for tile in tiles]
    low = (place & reach) == 0
    return [
        jnp.where(low, pltpu.roll(tile, size - reach, axis), pltpu.roll(tile, reach, axis))
        for tile in tiles
    ]


def sort_tiles(tiles):
    sub = lax.broadcasted_iota(jnp.int32, (SUBS, LANES), 0)
    lane = lax.broadcasted_iota(jnp.int32, (SUBS, LANES), 1)
    sub_bits = (len(tiles) - 1).bit_length()
    lane_bits = sub_bits + 3
    bits = lane_bits + 7
    spot = [v + (sub << sub_bits) + (lane << lane_bits) for v in range(len(tiles))]
    for size in range(1, bits + 1):
        for bit in range(size - 1, -1, -1):
            others = swap_partner(tiles, bit, sub_bits, lane_bits)
            new = []
            for at, tile, other in zip(spot, tiles, others):
                turn = (at >> bit) if size == bits else (at >> bit) ^ (at >> size)
                new.append(
                    jnp.where(
                        (turn & 1) == 0, jnp.minimum(tile, other), jnp.maximum(tile, other)
                    )
                )
            tiles = new
    return tiles


def steps_kernel(
    sizes,
    half_ref,
    rate_ref,
    cond_ref,
    rev_ref,
    class_ref,
    tissue_v,
    tissue_gates,
    tissue_diff,
    fibre_v,
    fibre_gates,
    fibre_diff,
    junc_owner,
    junc_fibre,
    junc_fcell,
    junc_tcell,
    junc_class,
    out_ref,
    volt,
    gate,
    pre,
    diff,
    rowhot,
    colhot,
    send,
    local,
    recv,
    zrecv,
    hsend,
    hrecv,
    coef,
    tissue_in,
    fibre_in,
    pad_a,
    pad_b,
    payload,
    dense,
    spread,
    hotrow,
    hotcol,
    gain,
    remote,
    sent_codes,
    got_codes,
    send_sem,
    recv_sem,
    hsend_sem,
    hrecv_sem,
    gate_sem,
    code_sems,
):
    slabs, planes, layers, yb, fb, cb, deep = sizes
    n = slabs * planes
    nt = layers * yb
    nq = nt + fb * cb
    gates = gate.shape[0]
    rows = SUBS * nt
    chunk = 2 * deep
    per = SUBS // deep
    groups = n // per
    wave = n // WAVES
    slab = lax.axis_index("slab")
    plane = lax.axis_index("plane")

    def device(k):
        return (flip_bits(slab, k // planes), flip_bits(plane, k % planes))

    loads = [
        pltpu.make_async_copy(tissue_gates, tissue_in, gate_sem.at[0]),
        pltpu.make_async_copy(fibre_gates, fibre_in, gate_sem.at[1]),
    ]
    for load in loads:
        load.start()
    barrier = pltpu.get_barrier_semaphore()
    zero = jnp.zeros((SUBS, LANES), jnp.float32)
    for par in range(2):
        for way in range(2):
            for i in range(yb):
                zrecv[par, way, i] = zero
            for i in range(fb + 1):
                hrecv[par, way, i] = zero
    for way in range(2):
        hsend[way, fb] = zero
    for k in range(1, n):
        pl.semaphore_signal(barrier, inc=1, device_id=device(k), device_id_type=MESH)

    for z in range(layers):
        for y in range(yb):
            volt[z * yb + y] = tissue_v[z, SUBS * y : SUBS * (y + 1), :]
            diff[z * yb + y] = time_step * tissue_diff[z, SUBS * y : SUBS * (y + 1), :]
    for f in range(fb):
        for c in range(cb):
            at = (slice(SUBS * f, SUBS * (f + 1)), slice(LANES * c, LANES * (c + 1)))
            volt[nt + f * cb + c] = fibre_v[at]
            diff[nt + f * cb + c] = time_step * fibre_diff[at]

    sub = lax.broadcasted_iota(jnp.int32, (SUBS, LANES), 0)
    lane = lax.broadcasted_iota(jnp.int32, (SUBS, LANES), 1)
    me = slab * planes + plane
    classes = class_ref.shape[0]
    codes = rows * LANES * classes
    lines = junc_owner.shape[0]
    blocks = lines // SUBS
    total = lines * LANES
    tiles = []
    for v in range(blocks):
        at = slice(SUBS * v, SUBS * (v + 1))
        fibre, along = junc_fibre[at], junc_fcell[at]
        row = (fibre // SUBS * cb + along // LANES) * SUBS + fibre % SUBS
        code = junc_tcell[at] * classes + junc_class[at]
        payload[at] = (row * LANES + along % LANES) * codes + code
        tiles.append((junc_owner[at] ^ me) * total + (v * SUBS + sub) * LANES + lane)
    tiles = sort_tiles(tiles)
    for v in range(blocks):
        pad_a[pl.ds(v, SUBS, stride=blocks), :] = tiles[v]
    pad_b[:, 0:lines] = pad_a[...].T
    fold = LANES // lines
    lined = None
    wide_lane = lax.broadcasted_iota(jnp.int32, (lines, LANES), 1)
    for i in range(fold):
        piece = pad_b[pl.ds(i, lines, stride=fold), :]
        piece = pltpu.roll(piece, lines * i, 1) if i > 0 else piece
        lined = piece if i == 0 else jnp.where(wide_lane >= lines * i, piece, lined)
    facts = []
    for v in range(blocks):
        key = lined[SUBS * v : SUBS * (v + 1)]
        spot = key % total
        fact = jnp.zeros((SUBS, LANES), jnp.int32)
        for r in range(lines):
            line = jnp.broadcast_to(payload[r : r + 1, :], (SUBS, LANES))
            fact = jnp.where(spot // LANES == r, axis_gather(line, spot % LANES, 1), fact)
        dense[v, 0] = fact // codes // LANES
        dense[v, 1] = fact // codes % LANES
        facts.append((key // total, (v * SUBS + sub + 1) * (2 * codes) + fact % codes + 1))
    for k in range(n):
        found = jnp.zeros((SUBS, LANES), jnp.int32)
        for owner, fact in facts:
            found = found + jnp.where(owner == k, fact, 0)
        reach = deep
        while reach < SUBS:
            found = found + pltpu.roll(found, reach, 0)
            reach *= 2
        sent_codes[k] = found[:deep] % (2 * codes)
        spread[k] = jnp.maximum(found[:deep] // (2 * codes) - 1, 0)
    got_codes[0] = sent_codes[0]

    pl.semaphore_wait(barrier, n - 1)
    for k in range(n - 1, 0, -1):
        pltpu.make_async_remote_copy(
            src_ref=sent_codes.at[k],
            dst_ref=got_codes.at[k],
            send_sem=code_sems.at[0],
            recv_sem=code_sems.at[1],
            device_id=device(k),
            device_id_type=MESH,
        ).start()

    def set_coef(k, carry):
        even = jnp.where(k % 2 == 0, 1.0, -1.0)
        half_cond = 0.5 * cond_ref[k]
        scaled = (-time_step * math.log2(math.e)) * rate_ref[k]
        coef[0, k] = half_ref[k]
        coef[1, k] = 1.5 * scaled
        coef[2, k] = 0.5 * scaled
        coef[3, k] = even * half_cond
        coef[4, k] = even * half_cond * rev_ref[k]
        coef[5, k] = even
        return carry[0] + half_cond, carry[1] + half_cond * rev_ref[k]

    zero_scalar = jnp.float32(0.0)
    sum_cond, sum_pull = lax.fori_loop(0, gates, set_coef, (zero_scalar, zero_scalar))

    places = lax.broadcasted_iota(jnp.int32, (rows, LANES), 0)
    columns = lax.broadcasted_iota(jnp.int32, (LANES, LANES), 0)

    def set_hot(k, kind, i, row, col):
        hot = places == jnp.broadcast_to(row, (rows, LANES))
        rowhot[k, kind * deep + i] = jnp.where(hot, 1.0, 0.0).astype(jnp.bfloat16)
        hot = columns == jnp.broadcast_to(col, (LANES, LANES))
        hot = jnp.where(hot, 1.0, 0.0).astype(jnp.bfloat16)
        colhot[k, kind, :, LANES * i : LANES * (i + 1)] = hot

    def gain_of(code):
        kind = code % classes
        out = jnp.zeros(code.shape, jnp.float32)
        for c in range(classes):
            out = jnp.where(kind == c, class_ref[c], out)
        return out

    def tall_tile(value):
        return jnp.concatenate([value] * (SUBS // deep), axis=0) if deep < SUBS else value

    @pl.loop(0, n)
    def _(k):
        spot = tall_tile(spread[k])
        row = jnp.zeros((SUBS, LANES), jnp.int32)
        col = row
        for v in range(blocks):
            here = spot // SUBS == v
            row = jnp.where(here, axis_gather(dense[v, 0], spot % SUBS, 0), row)
            col = jnp.where(here, axis_gather(dense[v, 1], spot % SUBS, 0), col)
        code = sent_codes[k]
        gain[k, deep:chunk] = jnp.where(code > 0, gain_of(code - 1), 0.0)
        for i in range(deep):
            set_hot(k, 1, i, row[i : i + 1], col[i : i + 1])

    for load in loads:
        load.wait()

    @pl.loop(0, gates)
    def _(k):
        sign = coef[5, k]
        for z in range(layers):
            for y in range(yb):
                old = tissue_in[k, z, SUBS * y : SUBS * (y + 1), :]
                gate[k, z * yb + y] = (old + old - 1.0) * sign
        for f in range(fb):
            for c in range(cb):
                old = fibre_in[k, SUBS * f : SUBS * (f + 1), LANES * c : LANES * (c + 1)]
                gate[k, nt + f * cb + c] = (old + old - 1.0) * sign

    far = pl.ds(1, n - 1)
    pltpu.make_async_copy(got_codes.at[far], got_codes.at[far], code_sems.at[1]).wait()
    pltpu.make_async_copy(sent_codes.at[far], sent_codes.at[far], code_sems.at[0]).wait()

    @pl.loop(0, n)
    def _(k):
        code = got_codes[k]
        cell = jnp.maximum(code - 1, 0) // classes
        gain[k, 0:deep] = jnp.where(code > 0, gain_of(code - 1), 0.0)
        remote[0, k] = cell // LANES
        remote[1, k] = cell % LANES
        for i in range(deep):
            set_hot(k, 0, i, cell[i : i + 1] // LANES, cell[i : i + 1] % LANES)

    for m in range(n * deep // SUBS):
        for kind in range(2):
            parts = [remote[kind, m * (SUBS // deep) + p] for p in range(SUBS // deep)]
            hotrow[kind, m] = jnp.concatenate(parts, axis=0) if len(parts) > 1 else parts[0]
        parts = [spread[m * (SUBS // deep) + p] for p in range(SUBS // deep)]
        hotcol[m] = jnp.concatenate(parts, axis=0) if len(parts) > 1 else parts[0]

    def lookup(base, row_at, col_at):
        out = zero
        for r in range(rows):
            line = volt[base + r // SUBS, r % SUBS : r % SUBS + 1, :]
            line = jnp.broadcast_to(line, (SUBS, LANES))
            out = jnp.where(row_at == r, axis_gather(line, col_at, 1), out)
        return out

    def junction_copy(k, par):
        return pltpu.make_async_remote_copy(
            src_ref=send.at[k],
            dst_ref=recv.at[par, k],
            send_sem=send_sem,
            recv_sem=recv_sem.at[par, k // wave],
            device_id=device(k),
            device_id_type=MESH,
        )

    def z_copy(way, par):
        first = (layers - 1) * yb if way == 0 else 0
        return pltpu.make_async_remote_copy(
            src_ref=volt.at[pl.ds(first, yb)],
            dst_ref=zrecv.at[par, way],
            send_sem=hsend_sem.at[way],
            recv_sem=hrecv_sem.at[par, way],
            device_id=(slab + 1 - 2 * way, plane),
            device_id_type=MESH,
        )

    def h_copy(way, par):
        return pltpu.make_async_remote_copy(
            src_ref=hsend.at[way],
            dst_ref=hrecv.at[par, way],
            send_sem=hsend_sem.at[2 + way],
            recv_sem=hrecv_sem.at[par, 2 + way],
            device_id=(slab, plane + 1 - 2 * way),
            device_id_type=MESH,
        )

    halos = (
        (z_copy, 0, slab < slabs - 1, slab > 0),
        (z_copy, 1, slab > 0, slab < slabs - 1),
        (h_copy, 0, plane < planes - 1, plane > 0),
        (h_copy, 1, plane > 0, plane < planes - 1),
    )

    def flag(condition):
        return jnp.where(condition, 1.0, 0.0)

    @pl.loop(0, STEPS)
    def _(step):
        par = step % 2
        own = [lookup(nt, dense[v, 0], dense[v, 1]) for v in range(blocks)]
        for m in range(groups - 1, -1, -1):
            tissue_part = lookup(0, hotrow[0, m], hotrow[1, m])
            spot = hotcol[m]
            fibre_part = zero
            for v in range(blocks):
                fibre_part = jnp.where(
                    spot // SUBS == v, axis_gather(own[v], spot % SUBS, 0), fibre_part
                )
            for p in range(per):
                at = slice(deep * p, deep * (p + 1))
                k = per * m + p
                send[k, 0:deep] = fibre_part[at]
                send[k, deep:chunk] = tissue_part[at]
                local[k, 0:deep] = tissue_part[at]
                local[k, deep:chunk] = fibre_part[at]
            if m < groups - 1:
                for p in range(per - 1, -1, -1):
                    junction_copy(per * (m + 1) + p, par).start()
        recv[par, 0] = send[0]
        for f in range(fb):
            hsend[0, f] = pltpu.roll(volt[nt + f * cb + cb - 1], 1, 1)
            hsend[1, f] = pltpu.roll(volt[nt + f * cb], LANES - 1, 1)
        for z in range(layers):
            hsend[0, fb, z : z + 1, :] = volt[z * yb + yb - 1, SUBS - 1 : SUBS, :]
            hsend[1, fb, z : z + 1, :] = volt[z * yb, 0:1, :]
        for p in range(per - 1, 0, -1):
            junction_copy(p, par).start()
        for build, way, sends, receives in halos:

            @pl.when(sends)
            def _():
                build(way, par).start()

        half_set = nq // 2
        for first in (0, half_set):

            @functools.partial(
                lax.fori_loop, 0, gates // UNROLL, init_val=(zero,) * (2 * half_set)
            )
            def sums(step_k, carry):
                carry = list(carry)
                for u in range(UNROLL):
                    k = step_k * UNROLL + u
                    half, base, slope, cond, pull = (coef[i, k] for i in range(5))
                    for i in range(half_set):
                        q = first + i
                        shifted = volt[q] - half
                        target = jnp.tanh(shifted)
                        factor = jnp.exp2(base + slope * jnp.tanh(0.5 * shifted))
                        new = target + (gate[k, q] - target) * factor
                        gate[k, q] = new
                        carry[2 * i] = carry[2 * i] + cond * new
                        carry[2 * i + 1] = carry[2 * i + 1] + pull * new
                return tuple(carry)

            for i in range(half_set):
                pre[first + i] = volt[first + i] * (sum_cond + sums[2 * i]) - (
                    sum_pull + sums[2 * i + 1]
                )

        at_left, at_right = lane == 0, lane == LANES - 1
        for z in range(layers):
            for y in range(yb):
                q = z * yb + y
                v = volt[q]
                near = jnp.where(at_left, 0.0, pltpu.roll(v, 1, 1))
                near = near + jnp.where(at_right, 0.0, pltpu.roll(v, LANES - 1, 1))
                above = pltpu.roll(volt[q - 1], 1, 0) if y > 0 else zero
                below = pltpu.roll(volt[q + 1], SUBS - 1, 0) if y < yb - 1 else zero
                near = near + jnp.where(sub == 0, above, pltpu.roll(v, 1, 0))
                near = near + jnp.where(sub == SUBS - 1, below, pltpu.roll(v, SUBS - 1, 0))
                count = jnp.where(at_left | at_right, 5.0, 6.0)
                if y == 0:
                    count = count - jnp.where(sub == 0, flag(plane == 0), 0.0)
                if y == yb - 1:
                    count = count - jnp.where(sub == SUBS - 1, flag(plane == planes - 1), 0.0)
                if z > 0:
                    near = near + volt[q - yb]
                else:
                    count = count - flag(slab == 0)
                if z < layers - 1:
                    near = near + volt[q + yb]
                else:
                    count = count - flag(slab == slabs - 1)
                pre[q] = v + diff[q] * (near - count * v) - time_step * pre[q]
        for f in range(fb):
            for c in range(cb):
                q = nt + f * cb + c
                v = volt[q]
                before = pltpu.roll(volt[q - 1], 1, 1) if c > 0 else zero
                after = pltpu.roll(volt[q + 1], LANES - 1, 1) if c < cb - 1 else zero
                near = jnp.where(at_left, before, pltpu.roll(v, 1, 1))
                near = near + jnp.where(at_right, after, pltpu.roll(v, LANES - 1, 1))
                count = jnp.full((SUBS, LANES), 2.0, jnp.float32)
                if c == 0:
                    count = count - jnp.where(at_left, flag(plane == 0), 0.0)
                if c == cb - 1:
                    count = count - jnp.where(at_right, flag(plane == planes - 1), 0.0)
                pre[q] = v + diff[q] * (near - count * v) - time_step * pre[q]

        sums = [jnp.zeros((2 * rows, LANES), jnp.float32) for _ in range(2)]
        for w in range(WAVES):
            span = pl.ds(w * wave + (1 if w == 0 else 0), wave - (1 if w == 0 else 0))
            pltpu.make_async_copy(
                recv.at[par, span], recv.at[par, span], recv_sem.at[par, w]
            ).wait()
            for kind in range(2):
                for k in range(w * wave, (w + 1) * wave):
                    flow = gain[k] * (recv[par, k] - local[k])
                    parts = []
                    for i in range(kind * deep, (kind + 1) * deep):
                        value = jnp.broadcast_to(flow[i : i + 1, :], (2 * SUBS, LANES))
                        high = value.astype(jnp.bfloat16)
                        low = (value - high.astype(jnp.float32)).astype(jnp.bfloat16)
                        hot = rowhot[k, i]
                        tall = rows // (2 * SUBS)
                        parts.append(
                            jnp.concatenate(
                                [jnp.concatenate([high] * tall, axis=0) * hot]
                                + [jnp.concatenate([low] * tall, axis=0) * hot],
                                axis=0,
                            )
                        )
                    wide = jnp.concatenate(parts, axis=1) if deep > 1 else parts[0]
                    sums[kind] = sums[kind] + lax.dot_general(
                        wide,
                        colhot[k, kind],
                        (((1,), (1,)), ((), ())),
                        preferred_element_type=jnp.float32,
                    )
        pltpu.make_async_copy(send.at[pl.ds(1, n - 1)], send.at[pl.ds(1, n - 1)], send_sem).wait()
        for build, way, sends, receives in halos:

            @pl.when(receives)
            def _():
                build(way, par).wait_recv()

            @pl.when(sends)
            def _():
                build(way, par).wait_send()

        new = []
        for z in range(layers):
            for y in range(yb):
                q = z * yb + y
                source = sums[0][SUBS * q : SUBS * (q + 1)]
                source = source + sums[0][rows + SUBS * q : rows + SUBS * (q + 1)]
                halo = zero
                if z == 0:
                    halo = halo + zrecv[par, 0, y]
                if z == layers - 1:
                    halo = halo + zrecv[par, 1, y]
                if y == 0:
                    row = jnp.broadcast_to(hrecv[par, 0, fb, z : z + 1, :], (SUBS, LANES))
                    halo = halo + jnp.where(sub == 0, row, 0.0)
                if y == yb - 1:
                    row = jnp.broadcast_to(hrecv[par, 1, fb, z : z + 1, :], (SUBS, LANES))
                    halo = halo + jnp.where(sub == SUBS - 1, row, 0.0)
                new.append(pre[q] + diff[q] * halo + time_step * source)
        for f in range(fb):
            for c in range(cb):
                q = f * cb + c
                source = sums[1][SUBS * q : SUBS * (q + 1)]
                source = source + sums[1][rows + SUBS * q : rows + SUBS * (q + 1)]
                halo = zero
                if c == 0:
                    halo = halo + jnp.where(at_left, hrecv[par, 0, f], 0.0)
                if c == cb - 1:
                    halo = halo + jnp.where(at_right, hrecv[par, 1, f], 0.0)
                new.append(pre[nt + q] + diff[nt + q] * halo + time_step * source)
        for q in range(nq):
            volt[q] = new[q]

    out_ref[...] = volt[...]


def body(
    tissue_v,
    tissue_gates,
    tissue_diff,
    fibre_v,
    fibre_gates,
    fibre_diff,
    gate_half,
    gate_rate,
    gate_cond,
    gate_rev,
    junc_cond,
    junc_fibre,
    junc_fcell,
    junc_owner,
    junc_tcell,
    junc_class,
):
    slabs = lax.axis_size("slab")
    planes = lax.axis_size("plane")
    n = slabs * planes
    layers, rows_dev, cols_dev = tissue_v.shape
    fibre_rows, fibre_cols = fibre_v.shape
    junctions = junc_fibre.shape[0]
    capacity = 2 * junctions // n
    deep = -(-capacity // LANES)
    chunk = 2 * deep
    yb, fb, cb = rows_dev // SUBS, fibre_rows // SUBS, fibre_cols // LANES
    nt = layers * yb
    nq = nt + fb * cb
    rows = nt * SUBS
    lines = junctions // LANES
    gates = gate_half.shape[0]
    per = SUBS // deep
    smem = pl.BlockSpec(memory_space=pltpu.SMEM)
    hbm = pl.BlockSpec(memory_space=pl.ANY)
    vmem = pl.BlockSpec(memory_space=pltpu.VMEM)
    flat = [
        x.reshape(lines, LANES) for x in (junc_owner, junc_fibre, junc_fcell, junc_tcell, junc_class)
    ]
    out = pl.pallas_call(
        functools.partial(steps_kernel, (slabs, planes, layers, yb, fb, cb, deep)),
        out_shape=jax.ShapeDtypeStruct((nq, SUBS, LANES), jnp.float32),
        in_specs=[smem] * 5 + [vmem, hbm, vmem, vmem, hbm, vmem] + [vmem] * 5,
        out_specs=vmem,
        scratch_shapes=[
            pltpu.VMEM((nq, SUBS, LANES), jnp.float32),
            pltpu.VMEM((gates, nq, SUBS, LANES), jnp.float32),
            pltpu.VMEM((nq, SUBS, LANES), jnp.float32),
            pltpu.VMEM((nq, SUBS, LANES), jnp.float32),
            pltpu.VMEM((n, chunk, rows, LANES), jnp.bfloat16),
            pltpu.VMEM((n, 2, LANES, deep * LANES), jnp.bfloat16),
            pltpu.VMEM((n, chunk, LANES), jnp.float32),
            pltpu.VMEM((n, chunk, LANES), jnp.float32),
            pltpu.VMEM((2, n, chunk, LANES), jnp.float32),
            pltpu.VMEM((2, 2, yb, SUBS, LANES), jnp.float32),
            pltpu.VMEM((2, fb + 1, SUBS, LANES), jnp.float32),
            pltpu.VMEM((2, 2, fb + 1, SUBS, LANES), jnp.float32),
            pltpu.SMEM((6, gates), jnp.float32),
            pltpu.VMEM(tissue_gates.shape, jnp.float32),
            pltpu.VMEM(fibre_gates.shape, jnp.float32),
            pltpu.VMEM((lines, LANES), jnp.int32),
            pltpu.VMEM((LANES, LANES), jnp.int32),
            pltpu.VMEM((lines, LANES), jnp.int32),
            pltpu.VMEM((lines // SUBS, 2, SUBS, LANES), jnp.int32),
            pltpu.VMEM((n, deep, LANES), jnp.int32),
            pltpu.VMEM((2, n // per, SUBS, LANES), jnp.int32),
            pltpu.VMEM((n // per, SUBS, LANES), jnp.int32),
            pltpu.VMEM((n, chunk, LANES), jnp.float32),
            pltpu.VMEM((2, n, deep, LANES), jnp.int32),
            pltpu.VMEM((n, deep, LANES), jnp.int32),
            pltpu.VMEM((n, deep, LANES), jnp.int32),
            pltpu.SemaphoreType.DMA,
            pltpu.SemaphoreType.DMA((2, WAVES)),
            pltpu.SemaphoreType.DMA((4,)),
            pltpu.SemaphoreType.DMA((2, 4)),
            pltpu.SemaphoreType.DMA((2,)),
            pltpu.SemaphoreType.DMA((2,)),
        ],
        compiler_params=pltpu.CompilerParams(
            collective_id=0, has_side_effects=True, vmem_limit_bytes=58 * 1024 * 1024
        ),
    )(
        gate_half,
        gate_rate,
        gate_cond,
        gate_rev,
        junc_cond,
        tissue_v,
        tissue_gates,
        tissue_diff,
        fibre_v,
        fibre_gates,
        fibre_diff,
        *flat,
    )
    fibre_out = out[nt:].reshape(fb, cb, SUBS, LANES).transpose(0, 2, 1, 3)
    return out[:nt].reshape(tissue_v.shape), fibre_out.reshape(fibre_v.shape)


def solution(mesh):
    in_specs = (
        P("slab", "plane", None),
        P(None, "slab", "plane", None),
        P("slab", "plane", None),
        P("slab", "plane"),
        P(None, "slab", "plane"),
        P("slab", "plane"),
        P(),
        P(),
        P(),
        P(),
        P(),
        P(("slab", "plane")),
        P(("slab", "plane")),
        P(("slab", "plane"), None),
        P(("slab", "plane")),
        P(("slab", "plane")),
    )
    out_specs = (P("slab", "plane", None), P("slab", "plane"))
    return jax.shard_map(body, mesh=mesh, in_specs=in_specs, out_specs=out_specs, check_vma=False)
```
